32 devices in a mesh: dp: 4 (over y, x), mp: 8 (over z, core).
Axes of the slice: x: 2, y: 2, z: 4, core: 2. Of those that a mesh axis runs over, the one named last changes fastest.
Arguments:
- data_rows: bfloat16 [16384, 2048], P(('dp', 'mp')), may hold values from -32 to 32
- centroids: bfloat16 [12288, 2048], P('mp'), may hold values from -0.75 to 0.75
- block_mask: int32 [8, 128], P(None, ('dp', 'mp')), may hold values from 0 to 1, as said below
- lower_bound: float32 [8, 16384], P(None, ('dp', 'mp')), may hold values from 0 to 4
Outputs:
- new_centroids: float32 [12288, 2048], P(('mp', 'dp'))
- centroid_shift: float32 [12288], P(('mp', 'dp'))
- log_norm: float32 [16384], P(('dp', 'mp'))
- new_lower: float32 [8, 16384], P(None, ('dp', 'mp'))
The draws below stay inside these ranges and needn't reach their ends.
Inputs may be any that keep to these rules, and one draw needn't show every extreme that they name: `block_mask`: within the 4 blocks of one device (aligned runs along the last dimension), at most 1 are 1 for each shard; for some shard every device has exactly 1.
All inputs are finite; a program needn't handle non-finite values.
Results may differ from the reference program's by a relative error of at most 0.0011.
Values may be sent and summed in bfloat16 or wider, within the bound.
A program may use at most 128 MiB of HBM per device.

```python
import math
import jax
import jax.numpy as jnp
from jax import lax

F = 2048
K = 12288
BLOCK = 128
SLOTS = 1
ROW_DEV = 512
ROWS = 16384
NBLOCKS = 128
N_MP = 8


def draw_masks(key):
    device_count = ROWS // ROW_DEV
    block_count = ROW_DEV // BLOCK
    base = jax.random.fold_in(key, 11)
    key_bits, key_heavy, key_forced, key_count = jax.random.split(base, 4)
    bits = jax.random.randint(key_bits, (device_count, N_MP, block_count), 0, 1 << 20)
    distinct = bits * block_count + jnp.arange(block_count, dtype=jnp.int32)[None, None, :]
    order = jnp.argsort(distinct, axis=-1)
    block_rank = jnp.argsort(order, axis=-1)
    heavy = jax.random.randint(key_heavy, (N_MP,), 0, 4) == 0
    forced = jax.random.randint(key_forced, (), 0, N_MP)
    heavy = heavy | (jnp.arange(N_MP) == forced)
    chosen_count = jax.random.randint(key_count, (device_count, N_MP), 0, SLOTS + 1)
    chosen_count = jnp.where(heavy[None, :], SLOTS, chosen_count)
    active = (block_rank < chosen_count[:, :, None]).astype(jnp.int32)
    return active.transpose(1, 0, 2).reshape(N_MP, NBLOCKS)


def draw_cents(key):
    base = jax.random.fold_in(key, 23)
    values = 0.125 * jax.random.normal(base, (K, F), jnp.float32)
    return jnp.clip(values, -0.75, 0.75)


def draw_block_mask(key, part):
    return draw_masks(key)


def draw_centroids(key, part):
    return draw_cents(key).astype(jnp.bfloat16)


def draw_data_rows(key, part):
    base = jax.random.fold_in(key, 37)
    key_main = jax.random.fold_in(base, 0)
    values = jnp.clip(jax.random.normal(key_main, (ROWS, F), jnp.float32), -6.0, 6.0)
    return values.astype(jnp.bfloat16)


def steps_of(rng, extent, shards, low, largest):
    def one(axis_at, blocks):
        draws = jax.random.uniform(jax.random.fold_in(jax.random.fold_in(rng, 6), axis_at), (blocks,), jnp.float32, low / len(shards), largest / len(shards))
        return jnp.repeat(jnp.exp(draws), extent[axis_at] // blocks).reshape((-1,) + (1,) * (len(extent) - axis_at - 1))

    level = one(*shards[0])
    for cut in shards[1:]:
        level = level * one(*cut)
    return level


def setup_inputs(seed: int = 0) -> dict:
    key_of = jax.random.split(jax.random.key(seed), 5)
    return {
        "data_rows": draw_data_rows(jax.random.fold_in(key_of[4], 71), 0),
        "centroids": draw_centroids(jax.random.fold_in(key_of[4], 71), 0),
        "block_mask": draw_block_mask(jax.random.fold_in(key_of[4], 71), 0),
        "lower_bound": jnp.clip(4.0 * jax.random.uniform(key_of[3], (N_MP, ROWS), jnp.float32) ** steps_of(key_of[3], (N_MP, ROWS), ((1, 32),), -0.2, 0.2), 0.0, 4.0),
    }


def pack_codes(mask_dev):
    block_count = mask_dev.shape[1]
    block_rank = (jnp.cumsum(mask_dev, axis=1) - 1).astype(jnp.int32)
    slot_ids = jnp.arange(SLOTS, dtype=jnp.int32)
    chosen = (mask_dev[:, None, :] == 1) & (block_rank[:, None, :] == slot_ids[None, :, None])
    labels = jnp.arange(1, block_count + 1, dtype=jnp.int32)
    return lax.optimization_barrier(jnp.sum(jnp.where(chosen, labels[None, None, :], 0), axis=2)).astype(jnp.int32)

def combine_rows(slot_codes, row_top, row_mass, block_count):
    labels = jnp.arange(1, block_count + 1, dtype=jnp.int32)
    is_slot = slot_codes[:, :, None] == labels[None, None, :]
    block_top = lax.optimization_barrier(jnp.max(jnp.where(is_slot[..., None], row_top[:, :, None, :], -1e+30), axis=(0, 1)))
    ceiling = jnp.maximum(block_top, 0.0)
    spread = row_mass[:, :, None, :] * jnp.exp(row_top[:, :, None, :] - ceiling[None, None])
    block_mass = lax.optimization_barrier(jnp.sum(jnp.where(is_slot[..., None], spread, 0.0), axis=(0, 1)))
    row_norm = ceiling + jnp.log(jnp.exp(-ceiling) + block_mass)
    slot_norm = lax.optimization_barrier(jnp.sum(jnp.where(is_slot[..., None], row_norm[None, None], 0.0), axis=2))
    return (row_norm, slot_norm)

def reference(data_rows, centroids, block_mask, lower_bound):
    device_count = ROWS // ROW_DEV
    block_count = ROW_DEV // BLOCK
    shard_width = K // N_MP
    sharpness = 4.0 / math.sqrt(F)
    row_blocks = data_rows.reshape(device_count, block_count, BLOCK, F)
    dev_mask = block_mask.reshape(N_MP, device_count, block_count).transpose(1, 0, 2)
    slot_codes = jax.vmap(pack_codes)(dev_mask)
    cents = centroids.reshape(N_MP, shard_width, F)
    cent_norm = lax.optimization_barrier(jnp.sum(jnp.square(cents.astype(jnp.float32)), axis=2))

    def slot_rows_of(shard):
        code_s = lax.dynamic_index_in_dim(slot_codes, shard, 1, keepdims=False)
        taken = jax.vmap(lambda blk, cde: jnp.take(blk, jnp.maximum(cde - 1, 0), axis=0))(row_blocks, code_s)
        return (jnp.where((code_s > 0)[:, :, None, None], taken, jnp.zeros_like(taken)), code_s)

    def shard_scores(shard):
        slot_rows, code_s = slot_rows_of(shard)
        cent_s = lax.dynamic_index_in_dim(cents, shard, 0, keepdims=False)
        norm_s = lax.dynamic_index_in_dim(cent_norm, shard, 0, keepdims=False)
        products = jnp.dot(slot_rows.reshape(-1, F), cent_s.T, preferred_element_type=jnp.float32)
        scores = sharpness * (2.0 * products - norm_s[None, :])
        scores = scores.reshape(device_count, SLOTS, BLOCK, shard_width)
        is_valid = (code_s > 0)[:, :, None]
        best = lax.optimization_barrier(jnp.max(scores, axis=3))
        row_top = jnp.where(is_valid, best, -1e+30)
        row_mass = jnp.where(is_valid, lax.optimization_barrier(jnp.sum(jnp.exp(scores - best[..., None]), axis=3)), 0.0)
        return (scores, row_top, row_mass)
    all_scores, all_top, all_mass = lax.map(shard_scores, jnp.arange(N_MP, dtype=jnp.int32))
    row_norm, slot_norm = jax.vmap(combine_rows, in_axes=(0, 1, 1, None))(slot_codes, all_top, all_mass, block_count)

    def shard_sums(shard):
        slot_rows, code_s = slot_rows_of(shard)
        scores = lax.dynamic_index_in_dim(all_scores, shard, 0, keepdims=False)
        norm_s = lax.dynamic_index_in_dim(slot_norm, shard, 1, keepdims=False)
        is_valid = (code_s > 0)[:, :, None, None]
        weight = jnp.where(is_valid, jnp.exp(scores - norm_s[..., None]), 0.0)
        counts = lax.optimization_barrier(jnp.sum(weight, axis=(0, 1, 2)))
        weight_half = weight.astype(jnp.bfloat16).reshape(-1, shard_width)
        weighted = jnp.dot(weight_half.T, slot_rows.reshape(-1, F), preferred_element_type=jnp.float32)
        return (weighted, counts)
    weighted, counts = lax.map(shard_sums, jnp.arange(N_MP, dtype=jnp.int32))
    old_cents = cents.astype(jnp.float32)
    updated = (weighted + old_cents) / (counts[..., None] + 1.0)
    movement = jnp.sqrt(lax.optimization_barrier(jnp.sum(jnp.square(updated - old_cents), axis=2)) + 1.0)
    shard_peak = lax.optimization_barrier(jnp.max(movement, axis=1))
    new_lower = lower_bound - shard_peak[:, None]
    return (updated.reshape(K, F), movement.reshape(K), row_norm.reshape(ROWS), new_lower)
```

```python
import functools
import math

import jax
import jax.numpy as jnp
from jax import lax
from jax.experimental import pallas as pl
from jax.experimental.pallas import tpu as pltpu
from jax.sharding import PartitionSpec as P

BLOCK = 128
SLOTS = 1
LOW = -1e30
MESH = pl.DeviceIdType.MESH
NT = (((1,), (1,)), ((), ()))


def xor(a, b, limit):
    out, bit = 0, 1
    while bit < limit:
        out = out + (((a // bit) % 2) + ((b // bit) % 2)) % 2 * bit
        bit *= 2
    return out


def skip_bit(j, stride):
    return j % stride + (j // stride) * 2 * stride


def kernel(dims, out_rows, codes, cents, upd, mv2, lognorm,
           x, cl, cn, s, w, st, gst, nm, norm, ct, cr, sb, rb,
           bar_l, sem_bs, sem_br, sem_fs, sem_fr, sem_ss, sem_sr,
           sem_ms, sem_mr, sem_rs, sem_rr, sem_ns, sem_nr):
    n_dp, n_mp, feat, ks, sharp, nblk, stride, cols = dims
    group = n_dp // 2
    np_ = 2 * n_mp
    nc = feat // cols
    d, m = lax.axis_index("dp"), lax.axis_index("mp")
    core = m % 2

    def pick(a, b, which):
        return a * (1 - which) + b * which

    def mate_of(which):
        return pick(xor(d, 1, n_dp), xor(d, stride, n_dp), which)

    mate = mate_of(core)

    def red(j):
        return pick(xor(d, skip_bit(j, 1), n_dp), xor(d, skip_bit(j, stride), n_dp), core)

    def owner(p):
        g, t = p % 2, p // 2
        return {"dp": pick(d, mate, g), "mp": xor(m, t, n_mp)}

    def scorer(p):
        g, t = p % 2, p // 2
        return {"dp": pick(d, mate_of((core + t) % 2), g), "mp": xor(m, t, n_mp)}

    barrier = pltpu.get_barrier_semaphore()
    partners = [owner(p) for p in range(1, np_)]
    partners += [scorer(p) for p in range(1, np_) if p % 2 and (p // 2) % 2]
    partners += [{"dp": red(j), "mp": m} for j in range(1, group)]
    for device in partners:
        pl.semaphore_signal(barrier, inc=1, device_id=device, device_id_type=MESH)

    own = pltpu.make_async_copy(out_rows.at[0], x.at[0], bar_l.at[0])
    own.start()
    loads = []
    for j in range(group):
        c = pltpu.make_async_copy(cents.at[red(j)], cl.at[pl.ds(j * ks, ks)], bar_l.at[1 + j])
        c.start()
        loads.append(c)
    pl.semaphore_wait(barrier, len(partners))

    def block_copy(t):
        return pltpu.make_async_remote_copy(
            src_ref=out_rows.at[t], dst_ref=x.at[2 * t], send_sem=sem_bs.at[t],
            recv_sem=sem_br.at[t], device_id={"dp": d, "mp": xor(m, t, n_mp)}, device_id_type=MESH)

    def forward(t):
        return pltpu.make_async_remote_copy(
            src_ref=x.at[2 * t], dst_ref=x.at[2 * t + 1], send_sem=sem_fs.at[t],
            recv_sem=sem_fr.at[t], device_id={"dp": mate, "mp": m}, device_id_type=MESH)

    def stat_copy(p):
        return pltpu.make_async_remote_copy(
            src_ref=st.at[p], dst_ref=gst.at[p], send_sem=sem_ss.at[p],
            recv_sem=sem_sr.at[p], device_id=owner(p), device_id_type=MESH)

    def norm_copy(p):
        return pltpu.make_async_remote_copy(
            src_ref=nm.at[p // 2], dst_ref=norm.at[p], send_sem=sem_ms.at[p],
            recv_sem=sem_mr.at[p], device_id=scorer(p), device_id_type=MESH)

    def sum_copy(j, c):
        return pltpu.make_async_remote_copy(
            src_ref=sb.at[j - 1, c], dst_ref=rb.at[j - 1, c], send_sem=sem_rs.at[j - 1, c],
            recv_sem=sem_rr.at[j - 1, c], device_id={"dp": red(j), "mp": m}, device_id_type=MESH)

    def count_copy(j):
        return pltpu.make_async_remote_copy(
            src_ref=ct.at[pl.ds(j * ks, ks)], dst_ref=cr.at[j - 1], send_sem=sem_ns.at[j - 1],
            recv_sem=sem_nr.at[j - 1], device_id={"dp": red(j), "mp": m}, device_id_type=MESH)

    for t in range(1, n_mp):
        block_copy(t).start()

    for c in loads:
        c.wait()
    own.wait()

    step = 16

    def norm_rows(i, _):
        r = pl.ds(pl.multiple_of(i * step, step), step)
        v = cl[r, :].astype(jnp.float32)
        cn[r, :] = jnp.broadcast_to(jnp.sum(v * v, axis=1, keepdims=True), (step, BLOCK))
        return 0

    forward(0).start()
    lax.fori_loop(0, cl.shape[0] // step, norm_rows, 0)

    def score(p):
        prod = lax.dot_general(cl[...], x[p], NT, preferred_element_type=jnp.float32)
        sc = sharp * (2.0 * prod - cn[...])
        s[p] = sc
        top = jnp.max(sc, axis=0, keepdims=True)
        st[p, 0:1, :] = top
        st[p, 1:2, :] = jnp.sum(jnp.exp(sc - top), axis=0, keepdims=True)

    score(0)

    def body(i, _):
        @pl.when(i < n_mp)
        def _():
            block_copy(i).wait_recv()
            forward(i).start()
            score(2 * i)
            stat_copy(2 * i).start()

        forward(i - 1).wait_recv()
        score(2 * i - 1)
        stat_copy(2 * i - 1).start()
        return 0

    lax.fori_loop(1, n_mp + 1, body, 0)
    gst[0] = st[0]
    for p in range(1, np_):
        stat_copy(p).wait_recv()

    mine = [codes[t:t + 1, :] for t in range(n_mp)]
    slot = [jnp.full((1, BLOCK), -LOW, jnp.float32) for _ in range(n_mp)]
    for b in range(nblk):
        top = jnp.zeros((1, BLOCK), jnp.float32)
        for p in range(np_):
            top = jnp.maximum(top, jnp.where(mine[p // 2] == b + 1, gst[p, 0:1, :], LOW))
        total = jnp.exp(-top)
        for p in range(np_):
            part = gst[p, 1:2, :] * jnp.exp(jnp.minimum(gst[p, 0:1, :] - top, 0.0))
            total = total + jnp.where(mine[p // 2] == b + 1, part, 0.0)
        val = top + jnp.log(total)
        lognorm[b:b + 1, :] = val
        slot = [jnp.where(mine[t] == b + 1, val, slot[t]) for t in range(n_mp)]
    for t in range(n_mp):
        nm[t] = slot[t]
    for p in range(1, np_):
        norm_copy(p).start()
    norm[0] = slot[0]
    for p in range(1, np_):
        norm_copy(p).wait_recv()

    ct[...] = jnp.zeros_like(ct)

    def weigh(p, _):
        wt = jnp.exp(s[p] - norm[p])
        ct[...] += wt
        w[:, pl.ds(pl.multiple_of(p * BLOCK, BLOCK), BLOCK)] = wt.astype(jnp.bfloat16)
        return 0

    lax.fori_loop(0, np_, weigh, 0)

    def partial(j, c):
        at = pl.ds(pl.multiple_of(c * cols, cols), cols)
        return jnp.dot(w[j * ks:(j + 1) * ks, :], x[:, :, at].reshape(np_ * BLOCK, cols),
                       preferred_element_type=jnp.float32)

    for j in range(1, group):
        count_copy(j).start()

        def send(c, _):
            sb[j - 1, c] = partial(j, c)
            sum_copy(j, c).start()
            return 0

        lax.fori_loop(0, nc, send, 0)
    cnt = ct[:ks]
    for j in range(1, group):
        count_copy(j).wait_recv()
        cnt = cnt + cr[j - 1]
    ct[:ks] = jnp.broadcast_to(jnp.sum(cnt, axis=1, keepdims=True) + 1.0, (ks, BLOCK))
    mv2[...] = jnp.zeros_like(mv2)

    def finish(c, _):
        at = pl.ds(pl.multiple_of(c * cols, cols), cols)
        total = partial(0, c)
        for j in range(1, group):
            sum_copy(j, c).wait_recv()
            total = total + rb[j - 1, c]
        old = cl[:ks, at].astype(jnp.float32)
        new = (total + old) / ct[:ks, :1]
        upd[:, at] = new
        mv2[...] += jnp.broadcast_to(
            jnp.sum(jnp.square(new - old), axis=1, keepdims=True), (ks, BLOCK))
        return 0

    lax.fori_loop(0, nc, finish, 0)

    for p in range(1, np_):
        stat_copy(p).wait_send()
        norm_copy(p).wait_send()
    for t in range(n_mp):
        if t:
            block_copy(t).wait_send()
        forward(t).wait_send()
    for j in range(1, group):
        count_copy(j).wait_send()
        for c in range(nc):
            sum_copy(j, c).wait_send()


def on_device(data_rows, centroids, block_mask, lower_bound):
    n_rows, feat = data_rows.shape
    nblk = n_rows // BLOCK
    n_dp, n_mp = lax.axis_size("dp"), lax.axis_size("mp")
    m = lax.axis_index("mp")
    ks = centroids.shape[0] // n_dp
    group, np_ = n_dp // 2, 2 * n_mp
    kc = group * ks
    stride = math.isqrt(n_dp)
    cols = 512
    nc = feat // cols
    labels = jnp.arange(1, nblk + 1, dtype=jnp.int32)
    order = jnp.bitwise_xor(jnp.arange(n_mp, dtype=jnp.int32), m)
    slot_codes = jnp.sum(jnp.take(block_mask, order, axis=0) * labels[None], axis=1)
    outgoing = jnp.take(data_rows.reshape(nblk, BLOCK, feat), jnp.maximum(slot_codes - 1, 0), axis=0)
    codes = jnp.broadcast_to(slot_codes[:, None], (n_mp, BLOCK))
    dims = (n_dp, n_mp, feat, ks, 4.0 / math.sqrt(feat), nblk, stride, cols)
    f32, bf16 = jnp.float32, jnp.bfloat16
    dma = pltpu.SemaphoreType.DMA
    vm = pl.BlockSpec(memory_space=pltpu.VMEM)
    hbm = pl.BlockSpec(memory_space=pl.ANY)
    upd, mv2, lognorm = pl.pallas_call(
        functools.partial(kernel, dims),
        out_shape=(
            jax.ShapeDtypeStruct((ks, feat), f32),
            jax.ShapeDtypeStruct((ks, BLOCK), f32),
            jax.ShapeDtypeStruct((nblk, BLOCK), f32),
        ),
        in_specs=[hbm, vm, hbm],
        out_specs=(vm, vm, vm),
        scratch_shapes=[
            pltpu.VMEM((np_, BLOCK, feat), bf16),
            pltpu.VMEM((kc, feat), bf16),
            pltpu.VMEM((kc, BLOCK), f32),
            pltpu.VMEM((np_, kc, BLOCK), f32),
            pltpu.VMEM((kc, np_ * BLOCK), bf16),
            pltpu.VMEM((np_, 2, BLOCK), f32),
            pltpu.VMEM((np_, 2, BLOCK), f32),
            pltpu.VMEM((n_mp, 1, BLOCK), f32),
            pltpu.VMEM((np_, 1, BLOCK), f32),
            pltpu.VMEM((kc, BLOCK), f32),
            pltpu.VMEM((group - 1, ks, BLOCK), f32),
            pltpu.VMEM((group - 1, nc, ks, cols), f32),
            pltpu.VMEM((group - 1, nc, ks, cols), f32),
            dma((1 + group,)),
            dma((n_mp,)), dma((n_mp,)),
            dma((n_mp,)), dma((n_mp,)),
            dma((np_,)), dma((np_,)),
            dma((np_,)), dma((np_,)),
            dma((group - 1, nc)), dma((group - 1, nc)),
            dma((group - 1,)), dma((group - 1,)),
        ],
        compiler_params=pltpu.CompilerParams(
            collective_id=0, has_side_effects=True, vmem_limit_bytes=60 * 1024 * 1024),
    )(outgoing, codes, centroids.reshape(n_dp, ks, feat))
    movement = jnp.sqrt(mv2[:, 0] + 1.0)
    shard_peaks = lax.all_gather(jnp.max(movement)[None], ("dp", "mp"), axis=0, tiled=True)
    shard_peak = jnp.max(shard_peaks.reshape(-1, n_mp), axis=0)
    return upd, movement, lognorm.reshape(-1), lower_bound - shard_peak[:, None]


def solution(mesh):
    placed = (P(("dp", "mp"), None), P("mp", None), P(None, ("dp", "mp")), P(None, ("dp", "mp")))
    return jax.shard_map(
        on_device,
        mesh=mesh,
        in_specs=placed,
        out_specs=(P(("mp", "dp"), None), P(("mp", "dp")), P(("dp", "mp")), P(None, ("dp", "mp"))),
        check_vma=False,
    )
```

```python
import functools
import math

import jax
import jax.numpy as jnp
from jax import lax
from jax.experimental import pallas as pl
from jax.experimental.pallas import tpu as pltpu
from jax.sharding import PartitionSpec as P

BLOCK = 128
SLOTS = 1
LOW = -1e30
MESH = pl.DeviceIdType.MESH
NT = (((1,), (1,)), ((), ()))


def xor(a, b, limit):
    out, bit = 0, 1
    while bit < limit:
        out = out + (((a // bit) % 2) + ((b // bit) % 2)) % 2 * bit
        bit *= 2
    return out


def skip_bit(j, stride):
    return j % stride + (j // stride) * 2 * stride


def kernel(dims, out_rows, codes, cents, lower, num, den, move, lognorm, newlow,
           x, cl, cn, s, w, st, gst, nm, norm, ct, cr, sb, rb, mv2, pk, gpk, apk,
           bar_l, sem_bs, sem_br, sem_fs, sem_fr, sem_ss, sem_sr,
           sem_ms, sem_mr, sem_rs, sem_rr, sem_ns, sem_nr, sem_ps, sem_pr, sem_as, sem_ar):
    n_dp, n_mp, feat, ks, sharp, nblk, stride, cols = dims
    group = n_dp // 2
    np_ = 2 * n_mp
    nc = feat // cols
    d, m = lax.axis_index("dp"), lax.axis_index("mp")
    core = m % 2

    def pick(a, b, which):
        return a * (1 - which) + b * which

    def mate_of(which):
        return pick(xor(d, 1, n_dp), xor(d, stride, n_dp), which)

    mate = mate_of(core)

    def red(j):
        return pick(xor(d, skip_bit(j, 1), n_dp), xor(d, skip_bit(j, stride), n_dp), core)

    def owner(p):
        g, t = p % 2, p // 2
        return {"dp": pick(d, mate, g), "mp": xor(m, t, n_mp)}

    def scorer(p):
        g, t = p % 2, p // 2
        return {"dp": pick(d, mate_of((core + t) % 2), g), "mp": xor(m, t, n_mp)}

    barrier = pltpu.get_barrier_semaphore()
    partners = [owner(p) for p in range(2, np_)]
    partners += [scorer(p) for p in range(1, np_) if p % 2 and (p // 2) % 2]
    partners += [{"dp": xor(d, e, n_dp), "mp": m} for e in range(1, n_dp)]
    for device in partners:
        pl.semaphore_signal(barrier, inc=1, device_id=device, device_id_type=MESH)

    own = pltpu.make_async_copy(out_rows.at[m], x.at[0], bar_l.at[0])
    own.start()
    loads = []
    for j in range(group):
        c = pltpu.make_async_copy(cents.at[red(j)], cl.at[pl.ds(j * ks, ks)], bar_l.at[1 + j])
        c.start()
        loads.append(c)
    pl.semaphore_wait(barrier, len(partners))

    def block_copy(t):
        return pltpu.make_async_remote_copy(
            src_ref=out_rows.at[xor(m, t, n_mp)], dst_ref=x.at[2 * t], send_sem=sem_bs.at[t],
            recv_sem=sem_br.at[t], device_id={"dp": d, "mp": xor(m, t, n_mp)}, device_id_type=MESH)

    def forward(t):
        return pltpu.make_async_remote_copy(
            src_ref=x.at[2 * t], dst_ref=x.at[2 * t + 1], send_sem=sem_fs.at[t],
            recv_sem=sem_fr.at[t], device_id={"dp": mate, "mp": m}, device_id_type=MESH)

    def stat_copy(p):
        return pltpu.make_async_remote_copy(
            src_ref=st.at[p], dst_ref=gst.at[p], send_sem=sem_ss.at[p],
            recv_sem=sem_sr.at[p], device_id=owner(p), device_id_type=MESH)

    def norm_copy(p):
        return pltpu.make_async_remote_copy(
            src_ref=nm.at[p // 2], dst_ref=norm.at[p], send_sem=sem_ms.at[p],
            recv_sem=sem_mr.at[p], device_id=scorer(p), device_id_type=MESH)

    def sum_copy(j, c):
        return pltpu.make_async_remote_copy(
            src_ref=sb.at[j - 1, c], dst_ref=rb.at[j - 1, c], send_sem=sem_rs.at[j - 1, c],
            recv_sem=sem_rr.at[j - 1, c], device_id={"dp": red(j), "mp": m}, device_id_type=MESH)

    def count_copy(j):
        return pltpu.make_async_remote_copy(
            src_ref=ct.at[pl.ds(j * ks, ks)], dst_ref=cr.at[j - 1], send_sem=sem_ns.at[j - 1],
            recv_sem=sem_nr.at[j - 1], device_id={"dp": red(j), "mp": m}, device_id_type=MESH)

    for t in range(1, n_mp):
        block_copy(t).start()

    for c in loads:
        c.wait()
    own.wait()

    step = 16

    def norm_rows(i, _):
        r = pl.ds(pl.multiple_of(i * step, step), step)
        v = cl[r, :].astype(jnp.float32)
        cn[r, :] = jnp.broadcast_to(jnp.sum(v * v, axis=1, keepdims=True), (step, BLOCK))
        return 0

    forward(0).start()
    lax.fori_loop(0, cl.shape[0] // step, norm_rows, 0)

    def score(p):
        prod = lax.dot_general(cl[...], x[p], NT, preferred_element_type=jnp.float32)
        sc = sharp * (2.0 * prod - cn[...])
        top = jnp.max(sc, axis=0, keepdims=True)
        ex = jnp.exp(sc - top)
        s[p] = ex
        st[p, 0:1, :] = top
        st[p, 1:2, :] = jnp.sum(ex, axis=0, keepdims=True)

    score(0)

    def body(i, _):
        @pl.when(i < n_mp)
        def _():
            block_copy(i).wait_recv()
            forward(i).start()
            score(2 * i)
            stat_copy(2 * i).start()

        forward(i - 1).wait_recv()
        score(2 * i - 1)
        stat_copy(2 * i - 1).start()
        return 0

    lax.fori_loop(1, n_mp + 1, body, 0)
    gst[0] = st[0]
    for p in range(1, np_):
        stat_copy(p).wait_recv()

    mine = [codes[pl.ds(xor(m, t, n_mp), 1), :] for t in range(n_mp)]
    slot = [jnp.full((1, BLOCK), -LOW, jnp.float32) for _ in range(n_mp)]
    for b in range(nblk):
        top = jnp.zeros((1, BLOCK), jnp.float32)
        for p in range(np_):
            top = jnp.maximum(top, jnp.where(mine[p // 2] == b + 1, gst[p, 0:1, :], LOW))
        total = jnp.exp(-top)
        for p in range(np_):
            part = gst[p, 1:2, :] * jnp.exp(jnp.minimum(gst[p, 0:1, :] - top, 0.0))
            total = total + jnp.where(mine[p // 2] == b + 1, part, 0.0)
        val = top + jnp.log(total)
        lognorm[b:b + 1, :] = val
        slot = [jnp.where(mine[t] == b + 1, val, slot[t]) for t in range(n_mp)]
    for t in range(n_mp):
        nm[t] = slot[t]
    for p in range(1, np_):
        norm_copy(p).start()
    norm[0] = slot[0]
    for p in range(1, np_):
        norm_copy(p).wait_recv()

    ct[...] = jnp.zeros_like(ct)

    def weigh(p, _):
        wt = s[p] * jnp.exp(st[p, 0:1, :] - norm[p])
        ct[...] += wt
        w[:, pl.ds(pl.multiple_of(p * BLOCK, BLOCK), BLOCK)] = wt.astype(jnp.bfloat16)
        return 0

    lax.fori_loop(0, np_, weigh, 0)

    def partial(j, c):
        at = pl.ds(pl.multiple_of(c * cols, cols), cols)
        return jnp.dot(w[j * ks:(j + 1) * ks, :], x[:, :, at].reshape(np_ * BLOCK, cols),
                       preferred_element_type=jnp.float32)

    for j in range(1, group):
        count_copy(j).start()

        def send(c, _):
            sb[j - 1, c] = partial(j, c)
            sum_copy(j, c).start()
            return 0

        lax.fori_loop(0, nc, send, 0)
    cnt = ct[:ks]
    for j in range(1, group):
        count_copy(j).wait_recv()
        cnt = cnt + cr[j - 1]
    ct[:ks] = jnp.broadcast_to(jnp.sum(cnt, axis=1, keepdims=True) + 1.0, (ks, BLOCK))
    mv2[...] = jnp.zeros_like(mv2)

    def finish(c, _):
        at = pl.ds(pl.multiple_of(c * cols, cols), cols)
        total = partial(0, c)
        for j in range(1, group):
            sum_copy(j, c).wait_recv()
            total = total + rb[j - 1, c]
        old = cl[:ks, at].astype(jnp.float32)
        top = total + old
        num[:, at] = top
        new = top / ct[:ks, :1]
        mv2[...] += jnp.broadcast_to(
            jnp.sum(jnp.square(new - old), axis=1, keepdims=True), (ks, BLOCK))
        return 0

    lax.fori_loop(0, nc, finish, 0)
    den[...] = ct[:ks]
    moved = jnp.sqrt(mv2[...] + 1.0)
    move[...] = moved
    pk[0] = jnp.max(moved, axis=0, keepdims=True)

    def peak_copy(e):
        return pltpu.make_async_remote_copy(
            src_ref=pk.at[0], dst_ref=gpk.at[e], send_sem=sem_ps.at[e], recv_sem=sem_pr.at[e],
            device_id={"dp": xor(d, e, n_dp), "mp": m}, device_id_type=MESH)

    def shard_copy(t):
        return pltpu.make_async_remote_copy(
            src_ref=pk.at[1], dst_ref=apk.at[t], send_sem=sem_as.at[t], recv_sem=sem_ar.at[t],
            device_id={"dp": d, "mp": xor(m, t, n_mp)}, device_id_type=MESH)

    for e in range(1, n_dp):
        peak_copy(e).start()
    best = pk[0]
    for e in range(1, n_dp):
        peak_copy(e).wait_recv()
        best = jnp.maximum(best, gpk[e])
    pk[1] = best
    for t in range(1, n_mp):
        shard_copy(t).start()
    apk[0] = best
    for t in range(n_mp):
        if t:
            shard_copy(t).wait_recv()
        row = pl.ds(xor(m, t, n_mp), 1)
        newlow[row, :] = lower[row, :] - apk[t][:, :1]

    for e in range(1, n_dp):
        peak_copy(e).wait_send()
    for t in range(1, n_mp):
        shard_copy(t).wait_send()
    for p in range(1, np_):
        stat_copy(p).wait_send()
        norm_copy(p).wait_send()
    for t in range(n_mp):
        if t:
            block_copy(t).wait_send()
        forward(t).wait_send()
    for j in range(1, group):
        count_copy(j).wait_send()
        for c in range(nc):
            sum_copy(j, c).wait_send()


def on_device(data_rows, centroids, block_mask, lower_bound):
    n_rows, feat = data_rows.shape
    nblk = n_rows // BLOCK
    n_dp, n_mp = lax.axis_size("dp"), lax.axis_size("mp")
    ks = centroids.shape[0] // n_dp
    group, np_ = n_dp // 2, 2 * n_mp
    kc = group * ks
    stride = math.isqrt(n_dp)
    cols = 512
    nc = feat // cols
    labels = jnp.arange(1, nblk + 1, dtype=jnp.int32)
    slot_codes = jnp.sum(block_mask * labels[None], axis=1)
    picks = jnp.maximum(slot_codes - 1, 0)
    outgoing = jnp.take(data_rows.reshape(nblk, BLOCK, feat), picks, axis=0, mode="clip")
    codes = jnp.broadcast_to(slot_codes[:, None], (n_mp, BLOCK))
    dims = (n_dp, n_mp, feat, ks, 4.0 / math.sqrt(feat), nblk, stride, cols)
    f32, bf16 = jnp.float32, jnp.bfloat16
    dma = pltpu.SemaphoreType.DMA
    vm = pl.BlockSpec(memory_space=pltpu.VMEM)
    hbm = pl.BlockSpec(memory_space=pl.ANY)
    num, den, move, lognorm, newlow = pl.pallas_call(
        functools.partial(kernel, dims),
        out_shape=(
            jax.ShapeDtypeStruct((ks, feat), f32),
            jax.ShapeDtypeStruct((ks, BLOCK), f32),
            jax.ShapeDtypeStruct((ks, BLOCK), f32),
            jax.ShapeDtypeStruct((nblk, BLOCK), f32),
            jax.ShapeDtypeStruct(lower_bound.shape, f32),
        ),
        in_specs=[hbm, vm, hbm, vm],
        out_specs=(vm,) * 5,
        scratch_shapes=[
            pltpu.VMEM((np_, BLOCK, feat), bf16),
            pltpu.VMEM((kc, feat), bf16),
            pltpu.VMEM((kc, BLOCK), f32),
            pltpu.VMEM((np_, kc, BLOCK), f32),
            pltpu.VMEM((kc, np_ * BLOCK), bf16),
            pltpu.VMEM((np_, 2, BLOCK), f32),
            pltpu.VMEM((np_, 2, BLOCK), f32),
            pltpu.VMEM((n_mp, 1, BLOCK), f32),
            pltpu.VMEM((np_, 1, BLOCK), f32),
            pltpu.VMEM((kc, BLOCK), f32),
            pltpu.VMEM((group - 1, ks, BLOCK), f32),
            pltpu.VMEM((group - 1, nc, ks, cols), f32),
            pltpu.VMEM((group - 1, nc, ks, cols), f32),
            pltpu.VMEM((ks, BLOCK), f32),
            pltpu.VMEM((2, 1, BLOCK), f32),
            pltpu.VMEM((n_dp, 1, BLOCK), f32),
            pltpu.VMEM((n_mp, 1, BLOCK), f32),
            dma((1 + group,)),
            dma((n_mp,)), dma((n_mp,)),
            dma((n_mp,)), dma((n_mp,)),
            dma((np_,)), dma((np_,)),
            dma((np_,)), dma((np_,)),
            dma((group - 1, nc)), dma((group - 1, nc)),
            dma((group - 1,)), dma((group - 1,)),
            dma((n_dp,)), dma((n_dp,)),
            dma((n_mp,)), dma((n_mp,)),
        ],
        compiler_params=pltpu.CompilerParams(
            collective_id=0, has_side_effects=True, vmem_limit_bytes=60 * 1024 * 1024),
    )(outgoing, codes, centroids.reshape(n_dp, ks, feat), lower_bound)
    return num / den[:, :1], move[:, 0], lognorm.reshape(-1), newlow


def solution(mesh):
    placed = (P(("dp", "mp"), None), P("mp", None), P(None, ("dp", "mp")), P(None, ("dp", "mp")))
    return jax.shard_map(
        on_device,
        mesh=mesh,
        in_specs=placed,
        out_specs=(P(("mp", "dp"), None), P(("mp", "dp")), P(("dp", "mp")), P(None, ("dp", "mp"))),
        check_vma=False,
    )
```

```python
import functools
import math

import jax
import jax.numpy as jnp
from jax import lax
from jax.experimental import pallas as pl
from jax.experimental.pallas import tpu as pltpu
from jax.sharding import PartitionSpec as P

BLOCK = 128
SLOTS = 1
HALVES = 2
LOW = -1e30
TINY = 1e-33
LEVELS = 32767.0
MESH = pl.DeviceIdType.MESH
NT = (((1,), (1,)), ((), ()))


def xor(a, b, limit):
    out, bit = 0, 1
    while bit < limit:
        out = out + (((a // bit) % 2) + ((b // bit) % 2)) % 2 * bit
        bit *= 2
    return out


def skip_bit(j, stride):
    return j % stride + (j // stride) * 2 * stride


def kernel(dims, out_rows, codes, cents, lower, num, den, move, lognorm, newlow,
           x, cl, cn, s, w, st, gst, nm, norm, ct, cs, cr, pf, sb, rb, mv2, pk, gpk, apk,
           bar_l, sem_bs, sem_br, sem_fs, sem_fr, sem_ss, sem_sr,
           sem_ms, sem_mr, sem_rs, sem_rr, sem_ns, sem_nr, sem_ps, sem_pr, sem_as, sem_ar):
    n_dp, n_mp, feat, ks, sharp, nblk, stride, cols = dims
    group = n_dp // 2
    np_ = 2 * n_mp
    nc = feat // cols
    d, m = lax.axis_index("dp"), lax.axis_index("mp")
    core = m % 2

    def pick(a, b, which):
        return a * (1 - which) + b * which

    def mate_of(which):
        return pick(xor(d, 1, n_dp), xor(d, stride, n_dp), which)

    mate = mate_of(core)

    def red(j):
        return pick(xor(d, skip_bit(j, 1), n_dp), xor(d, skip_bit(j, stride), n_dp), core)

    def owner(p):
        g, t = p % 2, p // 2
        return {"dp": pick(d, mate, g), "mp": xor(m, t, n_mp)}

    def scorer(p):
        g, t = p % 2, p // 2
        return {"dp": pick(d, mate_of((core + t) % 2), g), "mp": xor(m, t, n_mp)}

    barrier = pltpu.get_barrier_semaphore()
    partners = [owner(p) for p in range(2, np_)]
    partners += [scorer(p) for p in range(1, np_) if p % 2 and (p // 2) % 2]
    partners += [{"dp": xor(d, e, n_dp), "mp": m} for e in range(1, n_dp)]
    for device in partners:
        pl.semaphore_signal(barrier, inc=1, device_id=device, device_id_type=MESH)

    own = pltpu.make_async_copy(out_rows.at[m], x.at[0], bar_l.at[0])
    own.start()
    loads = []
    for j in range(group):
        c = pltpu.make_async_copy(cents.at[red(j)], cl.at[pl.ds(j * ks, ks)], bar_l.at[1 + j])
        c.start()
        loads.append(c)
    pl.semaphore_wait(barrier, len(partners))

    half = BLOCK // HALVES

    def block_copy(t, h):
        part = pl.ds(h * half, half)
        return pltpu.make_async_remote_copy(
            src_ref=out_rows.at[xor(m, t, n_mp), part], dst_ref=x.at[2 * t, part],
            send_sem=sem_bs.at[t, h], recv_sem=sem_br.at[t, h],
            device_id={"dp": d, "mp": xor(m, t, n_mp)}, device_id_type=MESH)

    def forward(t, h):
        part = pl.ds(h * half, half)
        return pltpu.make_async_remote_copy(
            src_ref=x.at[2 * t, part], dst_ref=x.at[2 * t + 1, part],
            send_sem=sem_fs.at[t, h], recv_sem=sem_fr.at[t, h],
            device_id={"dp": mate, "mp": m}, device_id_type=MESH)

    def stat_copy(p):
        return pltpu.make_async_remote_copy(
            src_ref=st.at[p], dst_ref=gst.at[p], send_sem=sem_ss.at[p],
            recv_sem=sem_sr.at[p], device_id=owner(p), device_id_type=MESH)

    def norm_copy(p):
        return pltpu.make_async_remote_copy(
            src_ref=nm.at[p // 2], dst_ref=norm.at[p], send_sem=sem_ms.at[p],
            recv_sem=sem_mr.at[p], device_id=scorer(p), device_id_type=MESH)

    def sum_copy(j, c):
        return pltpu.make_async_remote_copy(
            src_ref=sb.at[j - 1, c], dst_ref=rb.at[j - 1, c], send_sem=sem_rs.at[j - 1, c],
            recv_sem=sem_rr.at[j - 1, c], device_id={"dp": red(j), "mp": m}, device_id_type=MESH)

    def count_copy(j):
        return pltpu.make_async_remote_copy(
            src_ref=cs.at[j - 1], dst_ref=cr.at[j - 1], send_sem=sem_ns.at[j - 1],
            recv_sem=sem_nr.at[j - 1], device_id={"dp": red(j), "mp": m}, device_id_type=MESH)

    for t in range(1, n_mp):
        for h in range(HALVES):
            block_copy(t, h).start()

    for c in loads:
        c.wait()
    own.wait()

    step = 16

    def norm_rows(i, _):
        r = pl.ds(pl.multiple_of(i * step, step), step)
        v = cl[r, :].astype(jnp.float32)
        cn[r, :] = jnp.broadcast_to(jnp.sum(v * v, axis=1, keepdims=True), (step, BLOCK))
        return 0

    for h in range(HALVES):
        forward(0, h).start()
    lax.fori_loop(0, cl.shape[0] // step, norm_rows, 0)

    def score(p):
        prod = lax.dot_general(cl[...], x[p], NT, preferred_element_type=jnp.float32)
        sc = sharp * (2.0 * prod - cn[...])
        top = jnp.max(sc, axis=0, keepdims=True)
        ex = jnp.exp(sc - top)
        s[p] = ex
        st[p, 0:1, :] = top
        st[p, 1:2, :] = jnp.sum(ex, axis=0, keepdims=True)

    score(0)

    def body(i, _):
        @pl.when(i < n_mp)
        def _():
            for h in range(HALVES):
                block_copy(i, h).wait_recv()
                forward(i, h).start()
            score(2 * i)
            stat_copy(2 * i).start()

        for h in range(HALVES):
            forward(i - 1, h).wait_recv()
        score(2 * i - 1)
        stat_copy(2 * i - 1).start()
        return 0

    lax.fori_loop(1, n_mp + 1, body, 0)
    gst[0] = st[0]
    for p in range(1, np_):
        stat_copy(p).wait_recv()

    mine = [codes[pl.ds(xor(m, t, n_mp), 1), :] for t in range(n_mp)]
    slot = [jnp.full((1, BLOCK), -LOW, jnp.float32) for _ in range(n_mp)]
    for b in range(nblk):
        top = jnp.zeros((1, BLOCK), jnp.float32)
        for p in range(np_):
            top = jnp.maximum(top, jnp.where(mine[p // 2] == b + 1, gst[p, 0:1, :], LOW))
        total = jnp.exp(-top)
        for p in range(np_):
            part = gst[p, 1:2, :] * jnp.exp(jnp.minimum(gst[p, 0:1, :] - top, 0.0))
            total = total + jnp.where(mine[p // 2] == b + 1, part, 0.0)
        val = top + jnp.log(total)
        lognorm[b:b + 1, :] = val
        slot = [jnp.where(mine[t] == b + 1, val, slot[t]) for t in range(n_mp)]
    for t in range(n_mp):
        nm[t] = slot[t]
    for p in range(1, np_):
        norm_copy(p).start()
    norm[0] = slot[0]
    for p in range(1, np_):
        norm_copy(p).wait_recv()

    ct[...] = jnp.zeros_like(ct)

    def weigh(p, _):
        wt = s[p] * jnp.exp(st[p, 0:1, :] - norm[p])
        ct[...] += wt
        w[:, pl.ds(pl.multiple_of(p * BLOCK, BLOCK), BLOCK)] = wt.astype(jnp.bfloat16)
        return 0

    lax.fori_loop(0, np_, weigh, 0)

    def partial(j, c):
        at = pl.ds(pl.multiple_of(c * cols, cols), cols)
        return jnp.dot(w[j * ks:(j + 1) * ks, :], x[:, :, at].reshape(np_ * BLOCK, cols),
                       preferred_element_type=jnp.float32)

    lane = lax.broadcasted_iota(jnp.int32, (ks, BLOCK), 1)
    for j in range(1, group):
        def build(c, peak):
            val = partial(j, c)
            pf[c] = val
            return jnp.maximum(peak, jnp.max(jnp.abs(val), axis=1, keepdims=True))

        peak = lax.fori_loop(0, nc, build, jnp.full((ks, 1), TINY, jnp.float32))
        tally = jnp.sum(ct[j * ks:(j + 1) * ks], axis=1, keepdims=True)
        cs[j - 1] = jnp.where(lane < BLOCK // 2, tally, peak * (1.0 / LEVELS))
        count_copy(j).start()
        mv2[...] = jnp.broadcast_to(LEVELS / peak, (ks, BLOCK))

        def send(c, _):
            level = jnp.clip(jnp.round(pf[c] * mv2[:, :1]), -LEVELS, LEVELS)
            sb[j - 1, c] = level.astype(jnp.int32).astype(jnp.int16)
            sum_copy(j, c).start()
            return 0

        lax.fori_loop(0, nc, send, 0)
    cnt = jnp.sum(ct[:ks], axis=1, keepdims=True) + 1.0
    for j in range(1, group):
        count_copy(j).wait_recv()
        cnt = cnt + cr[j - 1, :, :1]
    ct[:ks] = jnp.broadcast_to(cnt, (ks, BLOCK))
    mv2[...] = jnp.zeros_like(mv2)

    def finish(c, _):
        at = pl.ds(pl.multiple_of(c * cols, cols), cols)
        total = partial(0, c)
        for j in range(1, group):
            sum_copy(j, c).wait_recv()
            total = total + rb[j - 1, c].astype(jnp.int32).astype(jnp.float32) * cr[j - 1, :, BLOCK - 1:]
        old = cl[:ks, at].astype(jnp.float32)
        top = total + old
        num[:, at] = top
        new = top / ct[:ks, :1]
        mv2[...] += jnp.broadcast_to(
            jnp.sum(jnp.square(new - old), axis=1, keepdims=True), (ks, BLOCK))
        return 0

    lax.fori_loop(0, nc, finish, 0)
    den[...] = ct[:ks]
    moved = jnp.sqrt(mv2[...] + 1.0)
    move[...] = moved
    pk[0] = jnp.max(moved, axis=0, keepdims=True)

    def peak_copy(e):
        return pltpu.make_async_remote_copy(
            src_ref=pk.at[0], dst_ref=gpk.at[e], send_sem=sem_ps.at[e], recv_sem=sem_pr.at[e],
            device_id={"dp": xor(d, e, n_dp), "mp": m}, device_id_type=MESH)

    def shard_copy(t):
        return pltpu.make_async_remote_copy(
            src_ref=pk.at[1], dst_ref=apk.at[t], send_sem=sem_as.at[t], recv_sem=sem_ar.at[t],
            device_id={"dp": d, "mp": xor(m, t, n_mp)}, device_id_type=MESH)

    for e in range(1, n_dp):
        peak_copy(e).start()
    best = pk[0]
    for e in range(1, n_dp):
        peak_copy(e).wait_recv()
        best = jnp.maximum(best, gpk[e])
    pk[1] = best
    for t in range(1, n_mp):
        shard_copy(t).start()
    apk[0] = best
    for t in range(n_mp):
        if t:
            shard_copy(t).wait_recv()
        row = pl.ds(xor(m, t, n_mp), 1)
        newlow[row, :] = lower[row, :] - apk[t][:, :1]

    for e in range(1, n_dp):
        peak_copy(e).wait_send()
    for t in range(1, n_mp):
        shard_copy(t).wait_send()
    for p in range(1, np_):
        stat_copy(p).wait_send()
        norm_copy(p).wait_send()
    for t in range(n_mp):
        for h in range(HALVES):
            if t:
                block_copy(t, h).wait_send()
            forward(t, h).wait_send()
    for j in range(1, group):
        count_copy(j).wait_send()
        for c in range(nc):
            sum_copy(j, c).wait_send()


def on_device(data_rows, centroids, block_mask, lower_bound):
    n_rows, feat = data_rows.shape
    nblk = n_rows // BLOCK
    n_dp, n_mp = lax.axis_size("dp"), lax.axis_size("mp")
    ks = centroids.shape[0] // n_dp
    group, np_ = n_dp // 2, 2 * n_mp
    kc = group * ks
    stride = math.isqrt(n_dp)
    cols = 256
    nc = feat // cols
    labels = jnp.arange(1, nblk + 1, dtype=jnp.int32)
    slot_codes = jnp.sum(block_mask * labels[None], axis=1)
    picks = jnp.maximum(slot_codes - 1, 0)
    outgoing = jnp.take(data_rows.reshape(nblk, BLOCK, feat), picks, axis=0, mode="clip")
    codes = jnp.broadcast_to(slot_codes[:, None], (n_mp, BLOCK))
    dims = (n_dp, n_mp, feat, ks, 4.0 / math.sqrt(feat), nblk, stride, cols)
    f32, bf16 = jnp.float32, jnp.bfloat16
    dma = pltpu.SemaphoreType.DMA
    vm = pl.BlockSpec(memory_space=pltpu.VMEM)
    hbm = pl.BlockSpec(memory_space=pltpu.HBM)
    num, den, move, lognorm, newlow = pl.pallas_call(
        functools.partial(kernel, dims),
        out_shape=(
            jax.ShapeDtypeStruct((ks, feat), f32),
            jax.ShapeDtypeStruct((ks, BLOCK), f32),
            jax.ShapeDtypeStruct((ks, BLOCK), f32),
            jax.ShapeDtypeStruct((nblk, BLOCK), f32),
            jax.ShapeDtypeStruct(lower_bound.shape, f32),
        ),
        in_specs=[hbm, vm, hbm, vm],
        out_specs=(vm,) * 5,
        scratch_shapes=[
            pltpu.VMEM((np_, BLOCK, feat), bf16),
            pltpu.VMEM((kc, feat), bf16),
            pltpu.VMEM((kc, BLOCK), f32),
            pltpu.VMEM((np_, kc, BLOCK), f32),
            pltpu.VMEM((kc, np_ * BLOCK), bf16),
            pltpu.VMEM((np_, 2, BLOCK), f32),
            pltpu.VMEM((np_, 2, BLOCK), f32),
            pltpu.VMEM((n_mp, 1, BLOCK), f32),
            pltpu.VMEM((np_, 1, BLOCK), f32),
            pltpu.VMEM((kc, BLOCK), f32),
            pltpu.VMEM((group - 1, ks, BLOCK), f32),
            pltpu.VMEM((group - 1, ks, BLOCK), f32),
            pltpu.VMEM((nc, ks, cols), f32),
            pltpu.VMEM((group - 1, nc, ks, cols), jnp.int16),
            pltpu.VMEM((group - 1, nc, ks, cols), jnp.int16),
            pltpu.VMEM((ks, BLOCK), f32),
            pltpu.VMEM((2, 1, BLOCK), f32),
            pltpu.VMEM((n_dp, 1, BLOCK), f32),
            pltpu.VMEM((n_mp, 1, BLOCK), f32),
            dma((1 + group,)),
            dma((n_mp, HALVES)), dma((n_mp, HALVES)),
            dma((n_mp, HALVES)), dma((n_mp, HALVES)),
            dma((np_,)), dma((np_,)),
            dma((np_,)), dma((np_,)),
            dma((group - 1, nc)), dma((group - 1, nc)),
            dma((group - 1,)), dma((group - 1,)),
            dma((n_dp,)), dma((n_dp,)),
            dma((n_mp,)), dma((n_mp,)),
        ],
        compiler_params=pltpu.CompilerParams(
            collective_id=0, has_side_effects=True, vmem_limit_bytes=44 * 1024 * 1024),
    )(outgoing, codes, centroids.reshape(n_dp, ks, feat), lower_bound)
    return num / den[:, :1], move[:, 0], lognorm.reshape(-1), newlow


def solution(mesh):
    placed = (P(("dp", "mp"), None), P("mp", None), P(None, ("dp", "mp")), P(None, ("dp", "mp")))
    return jax.shard_map(
        on_device,
        mesh=mesh,
        in_specs=placed,
        out_specs=(P(("mp", "dp"), None), P(("mp", "dp")), P(("dp", "mp")), P(None, ("dp", "mp"))),
        check_vma=False,
    )
```

```python
import functools
import math

import jax
import jax.numpy as jnp
from jax import lax
from jax.experimental import pallas as pl
from jax.experimental.pallas import tpu as pltpu
from jax.sharding import PartitionSpec as P

BLOCK = 128
SLOTS = 1
HALVES = 4
LOW = -1e30
TINY = 1e-33
LEVELS = 32767.0
MESH = pl.DeviceIdType.MESH
NT = (((1,), (1,)), ((), ()))


def xor(a, b, limit):
    out, bit = 0, 1
    while bit < limit:
        out = out + (((a // bit) % 2) + ((b // bit) % 2)) % 2 * bit
        bit *= 2
    return out


def skip_bit(j, stride):
    return j % stride + (j // stride) * 2 * stride


def kernel(dims, out_rows, codes, cents, lower, num, den, move, lognorm, newlow,
           x, cl, cn, s, w, st, gst, nm, norm, ct, cs, cr, pf, sb, rb, mv2, pk, gpk, apk,
           bar_l, sem_bs, sem_br, sem_fs, sem_fr, sem_ss, sem_sr,
           sem_ms, sem_mr, sem_rs, sem_rr, sem_ns, sem_nr, sem_ps, sem_pr, sem_as, sem_ar):
    n_dp, n_mp, feat, ks, sharp, nblk, stride, cols = dims
    group = n_dp // 2
    np_ = 2 * n_mp
    nc = feat // cols
    d, m = lax.axis_index("dp"), lax.axis_index("mp")
    core = m % 2

    def pick(a, b, which):
        return a * (1 - which) + b * which

    def mate_of(which):
        return pick(xor(d, 1, n_dp), xor(d, stride, n_dp), which)

    mate = mate_of(core)

    def red(j):
        return pick(xor(d, skip_bit(j, 1), n_dp), xor(d, skip_bit(j, stride), n_dp), core)

    def owner(p):
        g, t = p % 2, p // 2
        return {"dp": pick(d, mate, g), "mp": xor(m, t, n_mp)}

    def scorer(p):
        g, t = p % 2, p // 2
        return {"dp": pick(d, mate_of((core + t) % 2), g), "mp": xor(m, t, n_mp)}

    barrier = pltpu.get_barrier_semaphore()
    partners = [owner(p) for p in range(2, np_)]
    partners += [scorer(p) for p in range(1, np_) if p % 2 and (p // 2) % 2]
    partners += [{"dp": xor(d, e, n_dp), "mp": m} for e in range(1, n_dp)]
    for device in partners:
        pl.semaphore_signal(barrier, inc=1, device_id=device, device_id_type=MESH)

    own = pltpu.make_async_copy(out_rows.at[m], x.at[0], bar_l.at[0])
    own.start()
    loads = []
    for j in range(group):
        c = pltpu.make_async_copy(cents.at[red(j)], cl.at[pl.ds(j * ks, ks)], bar_l.at[1 + j])
        c.start()
        loads.append(c)
    pl.semaphore_wait(barrier, len(partners))

    half = BLOCK // HALVES

    def block_copy(t, h):
        part = pl.ds(h * half, half)
        return pltpu.make_async_remote_copy(
            src_ref=out_rows.at[xor(m, t, n_mp), part], dst_ref=x.at[2 * t, part],
            send_sem=sem_bs.at[t, h], recv_sem=sem_br.at[t, h],
            device_id={"dp": d, "mp": xor(m, t, n_mp)}, device_id_type=MESH)

    def forward(t, h):
        part = pl.ds(h * half, half)
        return pltpu.make_async_remote_copy(
            src_ref=x.at[2 * t, part], dst_ref=x.at[2 * t + 1, part],
            send_sem=sem_fs.at[t, h], recv_sem=sem_fr.at[t, h],
            device_id={"dp": mate, "mp": m}, device_id_type=MESH)

    def stat_copy(p):
        return pltpu.make_async_remote_copy(
            src_ref=st.at[p], dst_ref=gst.at[p], send_sem=sem_ss.at[p],
            recv_sem=sem_sr.at[p], device_id=owner(p), device_id_type=MESH)

    def norm_copy(p):
        return pltpu.make_async_remote_copy(
            src_ref=nm.at[p // 2], dst_ref=norm.at[p], send_sem=sem_ms.at[p],
            recv_sem=sem_mr.at[p], device_id=scorer(p), device_id_type=MESH)

    def sum_copy(j, c):
        return pltpu.make_async_remote_copy(
            src_ref=sb.at[j - 1, c], dst_ref=rb.at[j - 1, c], send_sem=sem_rs.at[j - 1, c],
            recv_sem=sem_rr.at[j - 1, c], device_id={"dp": red(j), "mp": m}, device_id_type=MESH)

    def count_copy(j):
        return pltpu.make_async_remote_copy(
            src_ref=cs.at[j - 1], dst_ref=cr.at[j - 1], send_sem=sem_ns.at[j - 1],
            recv_sem=sem_nr.at[j - 1], device_id={"dp": red(j), "mp": m}, device_id_type=MESH)

    for t in range(1, n_mp):
        for h in range(HALVES):
            block_copy(t, h).start()

    for c in loads:
        c.wait()
    own.wait()

    step = 16

    def norm_rows(i, _):
        r = pl.ds(pl.multiple_of(i * step, step), step)
        v = cl[r, :].astype(jnp.float32)
        cn[r, :] = jnp.broadcast_to(jnp.sum(v * v, axis=1, keepdims=True), (step, BLOCK))
        return 0

    for h in range(HALVES):
        forward(0, h).start()
    lax.fori_loop(0, cl.shape[0] // step, norm_rows, 0)

    def score(p):
        prod = lax.dot_general(cl[...], x[p], NT, preferred_element_type=jnp.float32)
        sc = sharp * (2.0 * prod - cn[...])
        top = jnp.max(sc, axis=0, keepdims=True)
        ex = jnp.exp(sc - top)
        s[p] = ex
        st[p, 0:1, :] = top
        st[p, 1:2, :] = jnp.sum(ex, axis=0, keepdims=True)

    score(0)

    def body(i, _):
        @pl.when(i < n_mp)
        def _():
            for h in range(HALVES):
                block_copy(i, h).wait_recv()
                forward(i, h).start()
            score(2 * i)
            stat_copy(2 * i).start()

        for h in range(HALVES):
            forward(i - 1, h).wait_recv()
        score(2 * i - 1)
        stat_copy(2 * i - 1).start()
        return 0

    lax.fori_loop(1, n_mp + 1, body, 0)
    gst[0] = st[0]
    for p in range(1, np_):
        stat_copy(p).wait_recv()

    mine = [codes[pl.ds(xor(m, t, n_mp), 1), :] for t in range(n_mp)]
    slot = [jnp.full((1, BLOCK), -LOW, jnp.float32) for _ in range(n_mp)]
    for b in range(nblk):
        top = jnp.zeros((1, BLOCK), jnp.float32)
        for p in range(np_):
            top = jnp.maximum(top, jnp.where(mine[p // 2] == b + 1, gst[p, 0:1, :], LOW))
        total = jnp.exp(-top)
        for p in range(np_):
            part = gst[p, 1:2, :] * jnp.exp(jnp.minimum(gst[p, 0:1, :] - top, 0.0))
            total = total + jnp.where(mine[p // 2] == b + 1, part, 0.0)
        val = top + jnp.log(total)
        lognorm[b:b + 1, :] = val
        slot = [jnp.where(mine[t] == b + 1, val, slot[t]) for t in range(n_mp)]
    for t in range(n_mp):
        nm[t] = slot[t]
    for p in range(1, np_):
        norm_copy(p).start()
    norm[0] = slot[0]
    for p in range(1, np_):
        norm_copy(p).wait_recv()

    ct[...] = jnp.zeros_like(ct)

    def weigh(j):
        rows = pl.ds(j * ks, ks)

        def one(p, _):
            wt = s[p, rows, :] * jnp.exp(st[p, 0:1, :] - norm[p])
            ct[rows, :] += wt
            w[rows, pl.ds(pl.multiple_of(p * BLOCK, BLOCK), BLOCK)] = wt.astype(jnp.bfloat16)
            return 0

        lax.fori_loop(0, np_, one, 0)

    def partial(j, c):
        at = pl.ds(pl.multiple_of(c * cols, cols), cols)
        return jnp.dot(w[j * ks:(j + 1) * ks, :], x[:, :, at].reshape(np_ * BLOCK, cols),
                       preferred_element_type=jnp.float32)

    lane = lax.broadcasted_iota(jnp.int32, (ks, BLOCK), 1)
    for j in range(1, group):
        def build(c, peak):
            val = partial(j, c)
            pf[c] = val
            return jnp.maximum(peak, jnp.max(jnp.abs(val), axis=1, keepdims=True))

        weigh(j)
        peak = lax.fori_loop(0, nc, build, jnp.full((ks, 1), TINY, jnp.float32))
        tally = jnp.sum(ct[j * ks:(j + 1) * ks], axis=1, keepdims=True)
        cs[j - 1] = jnp.where(lane < BLOCK // 2, tally, peak * (1.0 / LEVELS))
        count_copy(j).start()
        mv2[...] = jnp.broadcast_to(LEVELS / peak, (ks, BLOCK))

        def send(c, _):
            level = jnp.clip(jnp.round(pf[c] * mv2[:, :1]), -LEVELS, LEVELS)
            sb[j - 1, c] = level.astype(jnp.int32).astype(jnp.int16)
            sum_copy(j, c).start()
            return 0

        lax.fori_loop(0, nc, send, 0)
    weigh(0)
    cnt = jnp.sum(ct[:ks], axis=1, keepdims=True) + 1.0
    for j in range(1, group):
        count_copy(j).wait_recv()
        cnt = cnt + cr[j - 1, :, :1]
    ct[:ks] = jnp.broadcast_to(cnt, (ks, BLOCK))
    mv2[...] = jnp.zeros_like(mv2)

    def finish(c, _):
        at = pl.ds(pl.multiple_of(c * cols, cols), cols)
        total = partial(0, c)
        for j in range(1, group):
            sum_copy(j, c).wait_recv()
            total = total + rb[j - 1, c].astype(jnp.int32).astype(jnp.float32) * cr[j - 1, :, BLOCK - 1:]
        old = cl[:ks, at].astype(jnp.float32)
        top = total + old
        num[:, at] = top
        new = top / ct[:ks, :1]
        mv2[...] += jnp.broadcast_to(
            jnp.sum(jnp.square(new - old), axis=1, keepdims=True), (ks, BLOCK))
        return 0

    lax.fori_loop(0, nc, finish, 0)
    den[...] = ct[:ks]
    moved = jnp.sqrt(mv2[...] + 1.0)
    move[...] = moved
    pk[0] = jnp.max(moved, axis=0, keepdims=True)

    def peak_copy(e):
        return pltpu.make_async_remote_copy(
            src_ref=pk.at[0], dst_ref=gpk.at[e], send_sem=sem_ps.at[e], recv_sem=sem_pr.at[e],
            device_id={"dp": xor(d, e, n_dp), "mp": m}, device_id_type=MESH)

    def shard_copy(t):
        return pltpu.make_async_remote_copy(
            src_ref=pk.at[1], dst_ref=apk.at[t], send_sem=sem_as.at[t], recv_sem=sem_ar.at[t],
            device_id={"dp": d, "mp": xor(m, t, n_mp)}, device_id_type=MESH)

    for e in range(1, n_dp):
        peak_copy(e).start()
    best = pk[0]
    for e in range(1, n_dp):
        peak_copy(e).wait_recv()
        best = jnp.maximum(best, gpk[e])
    pk[1] = best
    for t in range(1, n_mp):
        shard_copy(t).start()
    apk[0] = best
    for t in range(n_mp):
        if t:
            shard_copy(t).wait_recv()
        row = pl.ds(xor(m, t, n_mp), 1)
        newlow[row, :] = lower[row, :] - apk[t][:, :1]

    for e in range(1, n_dp):
        peak_copy(e).wait_send()
    for t in range(1, n_mp):
        shard_copy(t).wait_send()
    for p in range(1, np_):
        stat_copy(p).wait_send()
        norm_copy(p).wait_send()
    for t in range(n_mp):
        for h in range(HALVES):
            if t:
                block_copy(t, h).wait_send()
            forward(t, h).wait_send()
    for j in range(1, group):
        count_copy(j).wait_send()
        for c in range(nc):
            sum_copy(j, c).wait_send()


def on_device(data_rows, centroids, block_mask, lower_bound):
    n_rows, feat = data_rows.shape
    nblk = n_rows // BLOCK
    n_dp, n_mp = lax.axis_size("dp"), lax.axis_size("mp")
    ks = centroids.shape[0] // n_dp
    group, np_ = n_dp // 2, 2 * n_mp
    kc = group * ks
    stride = math.isqrt(n_dp)
    cols = 256
    nc = feat // cols
    labels = jnp.arange(1, nblk + 1, dtype=jnp.int32)
    slot_codes = jnp.sum(block_mask * labels[None], axis=1)
    picks = jnp.maximum(slot_codes - 1, 0)
    outgoing = jnp.take(data_rows.reshape(nblk, BLOCK, feat), picks, axis=0, mode="clip")
    codes = jnp.broadcast_to(slot_codes[:, None], (n_mp, BLOCK))
    dims = (n_dp, n_mp, feat, ks, 4.0 / math.sqrt(feat), nblk, stride, cols)
    f32, bf16 = jnp.float32, jnp.bfloat16
    dma = pltpu.SemaphoreType.DMA
    vm = pl.BlockSpec(memory_space=pltpu.VMEM)
    hbm = pl.BlockSpec(memory_space=pltpu.HBM)
    num, den, move, lognorm, newlow = pl.pallas_call(
        functools.partial(kernel, dims),
        out_shape=(
            jax.ShapeDtypeStruct((ks, feat), f32),
            jax.ShapeDtypeStruct((ks, BLOCK), f32),
            jax.ShapeDtypeStruct((ks, BLOCK), f32),
            jax.ShapeDtypeStruct((nblk, BLOCK), f32),
            jax.ShapeDtypeStruct(lower_bound.shape, f32),
        ),
        in_specs=[hbm, vm, hbm, vm],
        out_specs=(vm,) * 5,
        scratch_shapes=[
            pltpu.VMEM((np_, BLOCK, feat), bf16),
            pltpu.VMEM((kc, feat), bf16),
            pltpu.VMEM((kc, BLOCK), f32),
            pltpu.VMEM((np_, kc, BLOCK), f32),
            pltpu.VMEM((kc, np_ * BLOCK), bf16),
            pltpu.VMEM((np_, 2, BLOCK), f32),
            pltpu.VMEM((np_, 2, BLOCK), f32),
            pltpu.VMEM((n_mp, 1, BLOCK), f32),
            pltpu.VMEM((np_, 1, BLOCK), f32),
            pltpu.VMEM((kc, BLOCK), f32),
            pltpu.VMEM((group - 1, ks, BLOCK), f32),
            pltpu.VMEM((group - 1, ks, BLOCK), f32),
            pltpu.VMEM((nc, ks, cols), f32),
            pltpu.VMEM((group - 1, nc, ks, cols), jnp.int16),
            pltpu.VMEM((group - 1, nc, ks, cols), jnp.int16),
            pltpu.VMEM((ks, BLOCK), f32),
            pltpu.VMEM((2, 1, BLOCK), f32),
            pltpu.VMEM((n_dp, 1, BLOCK), f32),
            pltpu.VMEM((n_mp, 1, BLOCK), f32),
            dma((1 + group,)),
            dma((n_mp, HALVES)), dma((n_mp, HALVES)),
            dma((n_mp, HALVES)), dma((n_mp, HALVES)),
            dma((np_,)), dma((np_,)),
            dma((np_,)), dma((np_,)),
            dma((group - 1, nc)), dma((group - 1, nc)),
            dma((group - 1,)), dma((group - 1,)),
            dma((n_dp,)), dma((n_dp,)),
            dma((n_mp,)), dma((n_mp,)),
        ],
        compiler_params=pltpu.CompilerParams(
            collective_id=0, has_side_effects=True, vmem_limit_bytes=44 * 1024 * 1024),
    )(outgoing, codes, centroids.reshape(n_dp, ks, feat), lower_bound)
    return num / den[:, :1], move[:, 0], lognorm.reshape(-1), newlow


def solution(mesh):
    placed = (P(("dp", "mp"), None), P("mp", None), P(None, ("dp", "mp")), P(None, ("dp", "mp")))
    return jax.shard_map(
        on_device,
        mesh=mesh,
        in_specs=placed,
        out_specs=(P(("mp", "dp"), None), P(("mp", "dp")), P(("dp", "mp")), P(None, ("dp", "mp"))),
        check_vma=False,
    )
```
